32 devices in a mesh: seg: 8 (over y, x, core), col: 4 (over z).
Axes of the slice: x: 2, y: 2, z: 4, core: 2. Of those that a mesh axis runs over, the one named last changes fastest.
Arguments:
- diagonal: float32 [32, 512, 512], P('seg', None, 'col'), as said below
- lower: float32 [32, 512, 512], P('seg'), as said below
- right_side: float32 [32, 512, 512], P('seg', None, 'col'), may hold values from -0.375 to 0.375
Outputs:
- solution: float32 [32, 512, 512], P('seg', None, 'col')
The draws below stay inside these ranges and needn't reach their ends.
Inputs may be any that keep to these rules, and one draw needn't show every extreme that they name: Every diagonal block is symmetric, and with lower it makes A symmetric positive definite. `lower`: with diagonal it makes A symmetric positive definite.
All inputs are finite; a program needn't handle non-finite values.
Results may differ from the reference program's by a relative error of at most 0.0003.
Values sent between devices are 32-bit elements; how exact they have to be, the bound alone decides.
A program may use at most 192 MiB of HBM per device.

```python
import math
import jax
import jax.numpy as jnp
from jax import lax

B = 512
K = 4
NRHS = 512
NB = 32


def chain_parts(key):
    base_key = jax.random.fold_in(key, 7)
    first_key, second_key, rate_key = jax.random.split(base_key, 3)
    noise_shape = (NB, B, B)
    first_noise = jax.random.normal(first_key, noise_shape, jnp.float32)
    second_noise = jax.random.normal(second_key, noise_shape, jnp.float32)
    decay_rates = jax.random.uniform(rate_key, (NB,), jnp.float32, 0.0, 0.1)
    carry_ratio = 1.0 - decay_rates / K
    identity = jnp.eye(B, dtype=jnp.float32)
    noise_scale = 0.3 / math.sqrt(B)
    upper_part = identity + noise_scale * first_noise
    lower_part = carry_ratio[:, None, None] * (identity + noise_scale * second_noise)
    return (upper_part, lower_part)


def draw_diagonal(key, part):
    upper_part, lower_part = chain_parts(key)
    gram_sum = jnp.einsum('nki,nkj->nij', upper_part, upper_part, precision=lax.Precision.HIGHEST)
    gram_sum = gram_sum + jnp.einsum('nki,nkj->nij', lower_part, lower_part, precision=lax.Precision.HIGHEST)
    gram_sum = 0.5 * (gram_sum + jnp.swapaxes(gram_sum, 1, 2))
    return gram_sum + 0.05 / (K * K) * jnp.eye(B, dtype=jnp.float32)


def draw_lower(key, part):
    upper_part, lower_part = chain_parts(key)
    shifted = jnp.roll(lower_part, 1, axis=0)
    return -jnp.einsum('nki,nkj->nij', upper_part, shifted, precision=lax.Precision.HIGHEST)


def shard_levels(rng, extent, shards, low, top_value):
    loudness = 1.0
    for position, shards_of in shards:
        steps = jax.random.uniform(jax.random.fold_in(jax.random.fold_in(rng, 6), position), (shards_of,), jnp.float32, low / len(shards), top_value / len(shards))
        loudness = loudness * jnp.repeat(jnp.exp(steps), extent[position] // shards_of).reshape((-1,) + (1,) * (len(extent) - 1 - position))
    return loudness


def centred(rng, shape, spread, limit, pieces=(), held_as=jnp.bfloat16):
    values = spread * jax.random.normal(rng, shape, jnp.float32)
    if pieces:
        values = values * shard_levels(rng, shape, pieces, -0.22, 0.18)
    return jnp.clip(values, -limit, limit).astype(held_as)


def setup_inputs(seed: int = 0) -> dict:
    streams_of = jax.random.split(jax.random.key(seed), 4)
    return {
        "diagonal": draw_diagonal(jax.random.fold_in(streams_of[3], 71), 0),
        "lower": draw_lower(jax.random.fold_in(streams_of[3], 71), 0),
        "right_side": centred(streams_of[2], (NB, B, NRHS), (1.0 / (K * K)), 0.375, ((0, 8), (2, 4)), jnp.float32),
    }


def matmul(left_hand, right_hand):
    return jnp.dot(left_hand.astype(jnp.float32), right_hand.astype(jnp.float32), precision=lax.Precision.HIGHEST, preferred_element_type=jnp.float32)

def chol_solve(factor, right_hand):
    halfway = lax.linalg.triangular_solve(factor, right_hand, left_side=True, lower=True)
    return lax.linalg.triangular_solve(factor, halfway, left_side=True, lower=True, transpose_a=True)

def reference(diagonal, lower, right_side):
    blocks = diagonal.shape[0]
    left_mask = (jnp.arange(blocks) > 0).astype(jnp.float32)[:, None, None]
    couple = lower * left_mask
    identity = jnp.eye(B, dtype=jnp.float32)

    def forward(state, inputs):
        factor, previous = state
        diag_block, coupling, rhs_block = inputs
        schur = diag_block - matmul(coupling, chol_solve(factor, coupling.T))
        new_factor = jnp.linalg.cholesky(schur)
        advanced = rhs_block - matmul(coupling, chol_solve(factor, previous))
        return ((new_factor, advanced), (new_factor, advanced))
    start_state = (identity, jnp.zeros((B, NRHS), jnp.float32))
    final_state, (factors, advanced) = lax.scan(forward, start_state, (diagonal, couple, right_side))
    next_links = jnp.concatenate([couple[1:], jnp.zeros((1, B, B), jnp.float32)], axis=0)

    def backward(later_block, inputs):
        factor, advanced_block, coupling = inputs
        solved = chol_solve(factor, advanced_block - matmul(coupling.T, later_block))
        return (solved, solved)
    last_state, solution = lax.scan(backward, jnp.zeros((B, NRHS), jnp.float32), (factors, advanced, next_links), reverse=True)
    return solution
```

```python
import jax
import jax.numpy as jnp
from jax import lax
from jax.experimental import pallas as pl
from jax.experimental.pallas import tpu as pltpu
from jax.sharding import PartitionSpec as P


def passed_along(shard, axis, by):
    size = lax.axis_size(axis)
    pairs = [(i, i + by) for i in range(size) if 0 <= i + by < size]
    return lax.ppermute(shard, axis, pairs)


def matmul(left_hand, right_hand):
    return jnp.dot(
        left_hand, right_hand, precision=lax.Precision.HIGHEST, preferred_element_type=jnp.float32
    )


TILE = 128
SUB = 8


def lanes_of(tile, lane):
    return jnp.broadcast_to(tile[:, lane : lane + 1], tile.shape)


def rows_of(tile, row):
    return jnp.broadcast_to(tile[row : row + 1, :], tile.shape)


def invert_tile(rows):
    lane = lax.broadcasted_iota(jnp.int32, (SUB, TILE), 1)
    sublane = lax.broadcasted_iota(jnp.int32, (SUB, TILE), 0)
    rows = list(rows)
    for panel in range(TILE // SUB):
        first = panel * SUB
        inside = (lane >= first) & (lane < first + SUB)
        own = rows[panel]
        inverse = [lanes_of(own, first + i) for i in range(SUB)]
        for r in range(SUB):
            at_r = sublane == r
            scale = 1.0 / rows_of(inverse[r], r)
            pivot = jnp.where(at_r, 1.0, inverse[r]) * scale
            for i in range(SUB):
                if i != r:
                    factor = rows_of(inverse[i], r)
                    inverse[i] = jnp.where(at_r, 0.0, inverse[i]) - factor * pivot
            inverse[r] = pivot
        marked = jnp.where(inside, (lane - first == sublane).astype(jnp.float32), own)
        swept = inverse[0] * rows_of(marked, 0)
        for i in range(1, SUB):
            swept = swept + inverse[i] * rows_of(marked, i)
        spread = [rows_of(swept, i) for i in range(SUB)]
        for t in range(TILE // SUB):
            if t != panel:
                total = jnp.where(inside, 0.0, rows[t])
                for i in range(SUB):
                    total = total - lanes_of(rows[t], first + i) * spread[i]
                rows[t] = total
        rows[panel] = swept
    return jnp.concatenate(rows, axis=0)


def invert_kernel(matrix_ref, out_ref):
    count, size = matrix_ref.shape[0], matrix_ref.shape[1]
    out_ref[...] = matrix_ref[...]
    eye = (
        lax.broadcasted_iota(jnp.int32, (TILE, TILE), 0)
        == lax.broadcasted_iota(jnp.int32, (TILE, TILE), 1)
    ).astype(jnp.float32)

    def step(k, carry):
        first = pl.multiple_of(k * TILE, TILE)
        here = pl.ds(first, TILE)
        tiles = []
        for m in range(count):
            rows = [
                out_ref[m, pl.ds(pl.multiple_of(first + t * SUB, SUB), SUB), here]
                for t in range(TILE // SUB)
            ]
            tiles.append(invert_tile(rows))
        for m in range(count):
            out_ref[m, here, here] = jnp.zeros((TILE, TILE), jnp.float32)
            column = out_ref[m, :, here]
            out_ref[m, :, here] = jnp.zeros((size, TILE), jnp.float32)
            out_ref[m, here, here] = eye
            swept = matmul(tiles[m], out_ref[m, here, :])
            out_ref[m] = out_ref[m] - matmul(column, swept)
            out_ref[m, here, :] = swept
        return carry

    lax.fori_loop(0, size // TILE, step, 0)


def invert_batch(matrices):
    count, size = matrices.shape[0], matrices.shape[1]
    return pl.pallas_call(
        invert_kernel,
        out_shape=jax.ShapeDtypeStruct(matrices.shape, jnp.float32),
        in_specs=[pl.BlockSpec(memory_space=pltpu.VMEM)],
        out_specs=pl.BlockSpec(memory_space=pltpu.VMEM),
        cost_estimate=pl.CostEstimate(
            flops=2 * count * size**3, bytes_accessed=8 * count * size**2, transcendentals=0
        ),
        compiler_params=pltpu.CompilerParams(vmem_limit_bytes=32 * 2**20),
        name="invert_spd",
    )(matrices)


def invert_spd(matrix):
    return invert_batch(matrix[None])[0]


def backward_sweep(inverses, next_links, advanced):

    def backward(later_block, inputs):
        inverse, advanced_block, coupling = inputs
        solved = matmul(inverse, advanced_block - matmul(coupling.T, later_block))
        return (solved, solved)

    last_state, solved = lax.scan(
        backward, jnp.zeros_like(advanced[0]), (inverses, advanced, next_links), reverse=True
    )
    return solved


def on_device(diagonal, lower, right_side):
    blocks = lower.shape[0]
    block_size = lower.shape[1]
    col_share = diagonal.shape[2]
    rhs_cols = right_side.shape[2]
    interior = blocks - 1
    offset = lax.axis_index("col") * col_share
    has_left = (lax.axis_index("seg") > 0).astype(jnp.float32)
    left_block = lower[0] * has_left
    sep_block = lower[blocks - 1]
    identity = jnp.eye(block_size, dtype=jnp.float32)
    left_mask = (jnp.arange(interior) > 0).astype(jnp.float32)[:, None, None]
    couple = lower[:interior] * left_mask
    next_links = jnp.concatenate(
        [couple[1:], jnp.zeros((1, block_size, block_size), jnp.float32)], axis=0
    )
    left_cols = lax.dynamic_slice_in_dim(left_block, offset, col_share, 1)
    right_cols = lax.dynamic_slice_in_dim(sep_block, offset, col_share, 0).T
    empty_cols = jnp.zeros((interior, block_size, col_share), jnp.float32)
    stacked = jnp.concatenate(
        [
            empty_cols.at[0].set(left_cols),
            empty_cols.at[interior - 1].set(right_cols),
            right_side[:interior],
        ],
        axis=2,
    )
    diag_items = lax.all_gather(diagonal[:interior], "col", axis=2, tiled=True)

    def forward(state, inputs):
        inverse, previous = state
        diag_block, coupling, rhs_block = inputs
        schur = diag_block - matmul(coupling, matmul(inverse, coupling.T))
        new_inverse = invert_spd(schur)
        advanced = rhs_block - matmul(coupling, matmul(inverse, previous))
        return ((new_inverse, advanced), (new_inverse, advanced))

    start_state = (identity, jnp.zeros((block_size, stacked.shape[2]), jnp.float32))
    final_state, (inverses, advanced) = lax.scan(
        forward, start_state, (diag_items, couple, stacked)
    )
    solved = backward_sweep(inverses, next_links, advanced)
    own_terms = matmul(sep_block, solved[interior - 1])
    next_terms = passed_along(matmul(left_block.T, solved[0]), "seg", -1)
    pivot_block = (
        diagonal[blocks - 1] - own_terms[:, col_share : 2 * col_share] - next_terms[:, :col_share]
    )
    sub_block = -own_terms[:, :col_share]
    super_block = -next_terms[:, col_share : 2 * col_share]
    reduced_rhs = (
        right_side[blocks - 1] - own_terms[:, 2 * col_share :] - next_terms[:, 2 * col_share :]
    )
    levels = (lax.axis_size("seg") - 1).bit_length()
    for level_bit in range(levels):
        stride = 1 << level_bit
        pivot_full, sub_full, super_full = (
            lax.all_gather(pivot_block, "col", axis=1, tiled=True),
            lax.all_gather(sub_block, "col", axis=1, tiled=True),
            lax.all_gather(super_block, "col", axis=1, tiled=True),
        )
        pivot_inverse = invert_spd(pivot_full)
        scaled = matmul(
            pivot_inverse, jnp.concatenate([sub_block, super_block, reduced_rhs], axis=1)
        )
        lower_terms = passed_along(scaled, "seg", stride)
        upper_terms = passed_along(scaled, "seg", -stride)
        narrow = sub_block.shape[1]
        new_sub = -matmul(sub_full, lower_terms[:, :narrow])
        new_super = -matmul(super_full, upper_terms[:, narrow : 2 * narrow])
        pivot_block = (
            pivot_block
            - matmul(sub_full, lower_terms[:, narrow : 2 * narrow])
            - matmul(super_full, upper_terms[:, :narrow])
        )
        reduced_rhs = (
            reduced_rhs
            - matmul(sub_full, lower_terms[:, 2 * narrow :])
            - matmul(super_full, upper_terms[:, 2 * narrow :])
        )
        sub_block, super_block = (new_sub, new_super)
    pivot_full = lax.all_gather(pivot_block, "col", axis=1, tiled=True)
    separator = matmul(invert_spd(pivot_full), reduced_rhs)
    left_sep = passed_along(separator, "seg", 1)
    correction = jnp.zeros((interior, block_size, rhs_cols), jnp.float32)
    correction = correction.at[0].add(matmul(left_block, left_sep))
    correction = correction.at[interior - 1].add(matmul(sep_block.T, separator))
    previous_inverses = jnp.concatenate([identity[None], inverses[:-1]], axis=0)

    def forward_only(previous, inputs):
        inverse, coupling, rhs_block = inputs
        advanced_block = rhs_block - matmul(coupling, matmul(inverse, previous))
        return (advanced_block, advanced_block)

    last_pushed, pushed = lax.scan(
        forward_only,
        jnp.zeros((block_size, rhs_cols), jnp.float32),
        (previous_inverses, couple, correction),
    )
    adjust = backward_sweep(inverses, next_links, pushed)
    interior_part = solved[:, :, 2 * col_share :] - adjust
    return jnp.concatenate([interior_part, separator[None]], axis=0)


def solution(mesh):
    in_specs = (P("seg", None, "col"), P("seg", None, None), P("seg", None, "col"))
    out_specs = P("seg", None, "col")
    return jax.shard_map(
        on_device, mesh=mesh, in_specs=in_specs, out_specs=out_specs, check_vma=False
    )
```

```python
import jax
import jax.numpy as jnp
from jax import lax
from jax.experimental import pallas as pl
from jax.experimental.pallas import tpu as pltpu
from jax.sharding import PartitionSpec as P


def passed_along(shard, axis, by):
    size = lax.axis_size(axis)
    pairs = [(i, i + by) for i in range(size) if 0 <= i + by < size]
    return lax.ppermute(shard, axis, pairs)


def matmul(left_hand, right_hand):
    return jnp.dot(
        left_hand, right_hand, precision=lax.Precision.HIGHEST, preferred_element_type=jnp.float32
    )


TILE = 128
SUB = 8


def lanes_of(tile, lane):
    return jnp.broadcast_to(tile[:, lane : lane + 1], tile.shape)


def rows_of(tile, row):
    return jnp.broadcast_to(tile[row : row + 1, :], tile.shape)


def invert_tile(rows):
    lane = lax.broadcasted_iota(jnp.int32, (SUB, TILE), 1)
    sublane = lax.broadcasted_iota(jnp.int32, (SUB, TILE), 0)
    rows = list(rows)
    for panel in range(TILE // SUB):
        first = panel * SUB
        inside = (lane >= first) & (lane < first + SUB)
        own = rows[panel]
        inverse = [lanes_of(own, first + i) for i in range(SUB)]
        for r in range(SUB):
            at_r = sublane == r
            scale = 1.0 / rows_of(inverse[r], r)
            pivot = jnp.where(at_r, 1.0, inverse[r]) * scale
            for i in range(SUB):
                if i != r:
                    factor = rows_of(inverse[i], r)
                    inverse[i] = jnp.where(at_r, 0.0, inverse[i]) - factor * pivot
            inverse[r] = pivot
        marked = jnp.where(inside, (lane - first == sublane).astype(jnp.float32), own)
        swept = inverse[0] * rows_of(marked, 0)
        for i in range(1, SUB):
            swept = swept + inverse[i] * rows_of(marked, i)
        spread = [rows_of(swept, i) for i in range(SUB)]
        for t in range(TILE // SUB):
            if t != panel:
                total = jnp.where(inside, 0.0, rows[t])
                for i in range(SUB):
                    total = total - lanes_of(rows[t], first + i) * spread[i]
                rows[t] = total
        rows[panel] = swept
    return jnp.concatenate(rows, axis=0)


def invert_kernel(matrix_ref, out_ref):
    count, size = matrix_ref.shape[0], matrix_ref.shape[1]
    out_ref[...] = matrix_ref[...]
    eye = (
        lax.broadcasted_iota(jnp.int32, (TILE, TILE), 0)
        == lax.broadcasted_iota(jnp.int32, (TILE, TILE), 1)
    ).astype(jnp.float32)

    def step(k, carry):
        first = pl.multiple_of(k * TILE, TILE)
        here = pl.ds(first, TILE)
        tiles = []
        for m in range(count):
            rows = [
                out_ref[m, pl.ds(pl.multiple_of(first + t * SUB, SUB), SUB), here]
                for t in range(TILE // SUB)
            ]
            tiles.append(invert_tile(rows))
        for m in range(count):
            out_ref[m, here, here] = jnp.zeros((TILE, TILE), jnp.float32)
            column = out_ref[m, :, here]
            out_ref[m, :, here] = jnp.zeros((size, TILE), jnp.float32)
            out_ref[m, here, here] = eye
            swept = matmul(tiles[m], out_ref[m, here, :])
            out_ref[m] = out_ref[m] - matmul(column, swept)
            out_ref[m, here, :] = swept
        return carry

    lax.fori_loop(0, size // TILE, step, 0)


def invert_batch(matrices):
    count, size = matrices.shape[0], matrices.shape[1]
    return pl.pallas_call(
        invert_kernel,
        out_shape=jax.ShapeDtypeStruct(matrices.shape, jnp.float32),
        in_specs=[pl.BlockSpec(memory_space=pltpu.VMEM)],
        out_specs=pl.BlockSpec(memory_space=pltpu.VMEM),
        cost_estimate=pl.CostEstimate(
            flops=2 * count * size**3, bytes_accessed=8 * count * size**2, transcendentals=0
        ),
        compiler_params=pltpu.CompilerParams(vmem_limit_bytes=32 * 2**20),
        name="invert_spd",
    )(matrices)


def invert_spd(matrix):
    return invert_batch(matrix[None])[0]


def on_device(diagonal, lower, right_side):
    blocks = lower.shape[0]
    block_size = lower.shape[1]
    col_share = diagonal.shape[2]
    interior = blocks - 1
    offset = lax.axis_index("col") * col_share
    has_left = (lax.axis_index("seg") > 0).astype(jnp.float32)
    left_block = lower[0] * has_left
    sep_block = lower[blocks - 1]
    assert interior == 3
    first_link, second_link = lower[1], lower[2]
    left_cols = lax.dynamic_slice_in_dim(left_block, offset, col_share, 1)
    right_cols = lax.dynamic_slice_in_dim(sep_block, offset, col_share, 0).T
    outer = jnp.concatenate([diagonal[0], diagonal[2]], axis=0)
    outer_full = lax.all_gather(outer, "col", axis=1, tiled=True)
    middle_full = lax.all_gather(diagonal[1], "col", axis=1, tiled=True)
    outer_inverses = invert_batch(outer_full.reshape(2, block_size, block_size))
    first_inverse, last_inverse = outer_inverses[0], outer_inverses[1]
    first_weight = matmul(first_link, first_inverse)
    last_weight = matmul(second_link.T, last_inverse)
    schur = (
        middle_full - matmul(first_weight, first_link.T) - matmul(last_weight, second_link)
    )
    middle_inverse = invert_spd(schur)
    first_rhs = jnp.concatenate([left_cols, right_side[0]], axis=1)
    last_rhs = jnp.concatenate([right_cols, right_side[2]], axis=1)
    first_push = matmul(first_weight, first_rhs)
    last_push = matmul(last_weight, last_rhs)
    middle_rhs = jnp.concatenate(
        [
            -first_push[:, :col_share],
            -last_push[:, :col_share],
            right_side[1] - first_push[:, col_share:] - last_push[:, col_share:],
        ],
        axis=1,
    )
    middle_solved = matmul(middle_inverse, middle_rhs)
    no_cols = jnp.zeros((block_size, col_share), jnp.float32)
    first_own = matmul(first_inverse, first_rhs)
    last_own = matmul(last_inverse, last_rhs)
    first_solved = jnp.concatenate(
        [first_own[:, :col_share], no_cols, first_own[:, col_share:]], axis=1
    ) - matmul(first_weight.T, middle_solved)
    last_solved = jnp.concatenate([no_cols, last_own], axis=1) - matmul(
        last_weight.T, middle_solved
    )
    own_terms = matmul(sep_block, last_solved)
    next_terms = passed_along(matmul(left_block.T, first_solved), "seg", -1)
    pivot_block = (
        diagonal[blocks - 1] - own_terms[:, col_share : 2 * col_share] - next_terms[:, :col_share]
    )
    sub_block = -own_terms[:, :col_share]
    super_block = -next_terms[:, col_share : 2 * col_share]
    reduced_rhs = (
        right_side[blocks - 1] - own_terms[:, 2 * col_share :] - next_terms[:, 2 * col_share :]
    )
    levels = (lax.axis_size("seg") - 1).bit_length()
    for level_bit in range(levels):
        stride = 1 << level_bit
        pivot_full, sub_full, super_full = (
            lax.all_gather(pivot_block, "col", axis=1, tiled=True),
            lax.all_gather(sub_block, "col", axis=1, tiled=True),
            lax.all_gather(super_block, "col", axis=1, tiled=True),
        )
        pivot_inverse = invert_spd(pivot_full)
        scaled = matmul(
            pivot_inverse, jnp.concatenate([sub_block, super_block, reduced_rhs], axis=1)
        )
        lower_terms = passed_along(scaled, "seg", stride)
        upper_terms = passed_along(scaled, "seg", -stride)
        narrow = sub_block.shape[1]
        new_sub = -matmul(sub_full, lower_terms[:, :narrow])
        new_super = -matmul(super_full, upper_terms[:, narrow : 2 * narrow])
        pivot_block = (
            pivot_block
            - matmul(sub_full, lower_terms[:, narrow : 2 * narrow])
            - matmul(super_full, upper_terms[:, :narrow])
        )
        reduced_rhs = (
            reduced_rhs
            - matmul(sub_full, lower_terms[:, 2 * narrow :])
            - matmul(super_full, upper_terms[:, 2 * narrow :])
        )
        sub_block, super_block = (new_sub, new_super)
    pivot_full = lax.all_gather(pivot_block, "col", axis=1, tiled=True)
    separator = matmul(invert_spd(pivot_full), reduced_rhs)
    left_sep = passed_along(separator, "seg", 1)
    first_fix = matmul(left_block, left_sep)
    last_fix = matmul(sep_block.T, separator)
    middle_fix = matmul(
        middle_inverse, matmul(first_weight, first_fix) + matmul(last_weight, last_fix)
    )
    return jnp.stack(
        [
            first_solved[:, 2 * col_share :]
            - matmul(first_inverse, first_fix)
            - matmul(first_weight.T, middle_fix),
            middle_solved[:, 2 * col_share :] + middle_fix,
            last_solved[:, 2 * col_share :]
            - matmul(last_inverse, last_fix)
            - matmul(last_weight.T, middle_fix),
            separator,
        ]
    )


def solution(mesh):
    in_specs = (P("seg", None, "col"), P("seg", None, None), P("seg", None, "col"))
    out_specs = P("seg", None, "col")
    return jax.shard_map(
        on_device, mesh=mesh, in_specs=in_specs, out_specs=out_specs, check_vma=False
    )
```
